128 devices in a mesh: member: 16 (over z, x_lo, core), space: 8 (over x_hi, y).
Axes of the slice: x: 4 (x_hi: 2, x_lo: 2; x = x_hi * 2 + x_lo), y: 4, z: 4, core: 2. Of those that a mesh axis runs over, the one named last changes fastest.
Arguments:
- weather: bfloat16 [16, 84, 256, 1440], P('member', None, 'space'), may hold values from -6 to 6
- coefficients: int32 [16, 84, 2, 368, 361], P('member', None, None, 'space'), may hold values from -1073741824 to 1073741823
- channel_scale: float32 [84], replicated, may hold values from 0.3 to 3
Outputs:
- perturbed: bfloat16 [16, 84, 256, 1440], P('member', None, 'space')
The draws below stay inside these ranges and needn't reach their ends.
All inputs are finite; a program needn't handle non-finite values.
Results may differ from the reference program's by a relative error of at most 0.007.
Values may be sent and summed in bfloat16 or wider, within the bound.
A program may use at most 192 MiB of HBM per device.

```python
import math
import jax
import jax.numpy as jnp
from jax import lax

CH = 84
LON = 1440
E = 16
LAT = 256
LAT0 = 232
LP = 361
MP = 368


def with_ends(values, rng, low, largest):
    longest = values.shape.index(max(values.shape))
    spots = []
    for shift in (0, 1):
        where = [jax.random.randint(jax.random.fold_in(rng, axis), (), 0, length) for axis, length in enumerate(values.shape)]
        where[longest] = (where[longest] + shift) % values.shape[longest]
        spots.append(tuple(where))
    return values.at[spots[0]].set(low).at[spots[1]].set(largest)


def shard_levels(key, extent, pieces, least, high):
    level = 1.0
    for position, blocks in pieces:
        heights = jax.random.uniform(jax.random.fold_in(jax.random.fold_in(key, 6), position), (blocks,), jnp.float32, least / len(pieces), high / len(pieces))
        level = level * jnp.repeat(jnp.exp(heights), extent[position] // blocks).reshape((-1,) + (1,) * (len(extent) - 1 - position))
    return level


def normal_values(own_key, dims, spread, reach, shards=(), kind=jnp.bfloat16):
    loudness = shard_levels(own_key, dims, shards, -0.22, 0.18) if shards else 1.0
    values = jax.random.normal(own_key, dims, jnp.float32) * spread * loudness
    return jnp.minimum(jnp.maximum(values, -reach), reach).astype(kind)


def setup_inputs(seed: int = 0) -> dict:
    key_list = jax.random.split(jax.random.key(seed), 4)
    weather = normal_values(key_list[0], (E, CH, LAT, LON), 1.0, 6.0, ((0, 16), (2, 8)))
    coefficients = with_ends(jax.random.randint(key_list[1], (E, CH, 2, MP, LP), -1073741824, 1073741824), jax.random.fold_in(key_list[1], 1), -1073741824, 1073741823).astype(jnp.int32)
    channel_scale = jnp.clip(jnp.exp(jax.random.uniform(key_list[2], (CH,), jnp.float32, math.log(0.3), math.log(3.0))), 0.3, 3.0)
    return dict(weather=weather, coefficients=coefficients, channel_scale=channel_scale)


def diagonal_log(order_count):
    steps_up = jnp.arange(1, order_count, dtype=jnp.int32).astype(jnp.float32)
    terms = 0.5 * jnp.log((2.0 * steps_up + 1.0) / (2.0 * steps_up))
    return jnp.concatenate([jnp.zeros((1,), jnp.float32), jnp.cumsum(terms)])

def legendre_table(orders, colatitude, order_logs, degree_count):
    order_values = orders.astype(jnp.float32)[:, None]
    cosine = jnp.cos(colatitude)[None, :]
    sine_values = jnp.sin(colatitude)[None, :]
    diagonal = jnp.exp(order_logs[:, None] - 0.5 * math.log(4.0 * math.pi) + order_values * jnp.log(sine_values))
    block_size = 16
    turn_count = (degree_count + block_size - 1) // block_size
    order_square = order_values * order_values

    def advance(carry, turn_index):
        older_row, newer_row = carry
        produced = []
        for inner_step in range(block_size):
            degree = (turn_index * block_size + inner_step).astype(jnp.float32)
            degree_square = degree * degree
            prior = degree - 1.0
            factor_up = jnp.sqrt(jnp.maximum(4.0 * degree_square - 1.0, 1.0) / jnp.maximum(degree_square - order_square, 1.0))
            factor_down = jnp.sqrt(jnp.maximum(prior * prior - order_square, 0.0) / jnp.maximum(4.0 * prior * prior - 1.0, 1.0))
            next_row = factor_up * (cosine * newer_row - factor_down * older_row)
            next_row = jnp.where(degree < order_values, 0.0, jnp.where(degree == order_values, diagonal, next_row))
            produced.append(next_row)
            older_row, newer_row = (newer_row, next_row)
        return ((older_row, newer_row), jnp.stack(produced))
    empty = jnp.zeros_like(diagonal)
    carried, stacked = lax.scan(advance, (empty, empty), jnp.arange(turn_count, dtype=jnp.int32))
    return stacked.reshape(turn_count * block_size, orders.shape[0], colatitude.shape[0])[:degree_count]

def spectral_values(coefficients, orders):
    degree_count = coefficients.shape[-1]
    degrees = jnp.arange(degree_count, dtype=jnp.int32)
    keep = degrees[None, :] >= orders[:, None]
    factor = math.sqrt(3.0) * math.sqrt(4.0 * math.pi) / degree_count * 2.0 ** (-30)
    values = coefficients.astype(jnp.float32) * factor
    return jnp.where(keep, values, 0.0).astype(jnp.bfloat16)

def fourier_basis(order_count, lon_count):
    orders = jnp.arange(order_count, dtype=jnp.int32)
    columns = jnp.arange(lon_count, dtype=jnp.int32)
    phases = orders[:, None] * columns[None, :] % lon_count
    angles = 2.0 * math.pi / lon_count * phases.astype(jnp.float32)
    weights = jnp.where(orders == 0, 1.0, math.sqrt(2.0)).astype(jnp.float32)[:, None]
    return jnp.stack([weights * jnp.cos(angles), weights * jnp.sin(angles)]).astype(jnp.bfloat16)

def reference(weather, coefficients, channel_scale):
    orders = jnp.arange(MP, dtype=jnp.int32)
    colatitude = math.pi * (LAT0 + jnp.arange(LAT, dtype=jnp.int32)).astype(jnp.float32) / (LON // 2)
    legendre = legendre_table(orders, colatitude, diagonal_log(MP), LP).astype(jnp.bfloat16)
    legendre_wide = lax.optimization_barrier(legendre).astype(jnp.float32)
    basis = fourier_basis(MP, LON).reshape(2 * MP, LON)

    def one_member(coef_member):
        spectral = lax.optimization_barrier(spectral_values(coef_member, orders)).astype(jnp.float32)
        fourier = jnp.einsum('cpml,lmt->ctpm', spectral, legendre_wide, precision=lax.Precision.HIGHEST).astype(jnp.bfloat16)
        noise = jnp.dot(fourier.reshape(CH * LAT, 2 * MP), basis, preferred_element_type=jnp.float32)
        return noise.astype(jnp.bfloat16).reshape(CH, LAT, LON)
    noise_all = lax.map(one_member, coefficients)

    def add_up(total, noise_member):
        return (total + noise_member.astype(jnp.float32), None)
    total, unused = lax.scan(add_up, jnp.zeros((CH, LAT, LON), jnp.float32), noise_all)
    mean = total / E

    def perturb(pair):
        weather_member, noise_member = pair
        centred = noise_member.astype(jnp.float32) - mean
        return (weather_member.astype(jnp.float32) + channel_scale[:, None, None] * centred).astype(jnp.bfloat16)
    return lax.map(perturb, (weather, noise_all))
```

```python
import functools
import math

import jax
import jax.numpy as jnp
import numpy as np
from jax import lax
from jax.experimental import pallas as pl
from jax.experimental.pallas import tpu as pltpu
from jax.sharding import PartitionSpec as P

MESH = pl.DeviceIdType.MESH
F32 = jnp.float32
BF16 = jnp.bfloat16
CB = 12
GR = CB // 4
LPAD = 384


def seeds(order_local, shards, lat, lat0, lon):
    rows = order_local + 2
    m_all = np.arange(shards * order_local + 8, dtype=np.float64)
    steps = np.maximum(m_all, 1.0)
    terms = np.where(m_all > 0, 0.5 * np.log((2.0 * steps + 1.0) / (2.0 * steps)), 0.0)
    logs = np.cumsum(terms) - 0.5 * math.log(4.0 * math.pi)
    index = order_local * np.arange(shards)[:, None] + np.arange(rows)[None, :]
    diag = np.broadcast_to(logs[index].reshape(-1, 1), (shards * rows, 128))
    colat = math.pi * (lat0 + np.arange(lat)) / (lon // 2)
    angle = np.broadcast_to(
        np.stack([np.cos(colat), np.log(np.sin(colat))])[:, None, :], (2, 8, lat)
    )
    degree = np.arange(LPAD, dtype=np.float64)
    factors = np.stack(
        [
            np.sqrt(np.maximum(4.0 * degree**2 - 1.0, 1.0)),
            1.0 / np.sqrt(np.maximum(4.0 * (degree - 1.0) ** 2 - 1.0, 1.0)),
        ]
    )
    lane = np.arange(1536)
    theta = np.where(lane < lon, 2.0 * math.pi * lane / lon, 0.0)[None, :]
    m = (np.arange(8) // 2)[:, None]
    p = (np.arange(8) % 2)[:, None]
    turn = []
    for by in (4, order_local):
        turn += [np.broadcast_to(f(by * theta), (8, 1536)) for f in (np.cos, np.sin)]
    wave = np.stack([np.cos(m * theta - p * math.pi / 2), np.sin(m * theta - p * math.pi / 2)] + turn)
    return [np.asarray(a, np.float32) for a in (diag, angle, factors, wave)]


def kernel(
    dims, weather, coefs, scale, diag, angle, factors, wave, out,
    cbuf, stage, table, four, held, hsend, hrecv, zsend, zrecv, xsend, xrecv,
    msend, mrecv, aown, apar, got, rows, basis, field,
    csem, wsem, osem, hs, hr, zs, zr, xs, xr, ms, mr, sown, spar, ar,
):
    chunks, order_local, degrees, lat, lon, shards, factor = dims
    half = shards // 2
    me = lax.axis_index("member")
    sp = lax.axis_index("space")
    core = lax.rem(me, 2)
    other = me + 1 - 2 * core
    across = me + 2 - 4 * lax.rem(me // 2, 2)
    zpos = me // 4
    ring = [lax.rem(zpos + j, 4) * 4 + lax.rem(me, 4) for j in range(4)]
    mine = core * half
    theirs = (1 - core) * half

    barrier = pltpu.get_barrier_semaphore()
    for j in range(1, 4):
        pl.semaphore_signal(barrier, inc=1, device_id=(ring[j], sp), device_id_type=MESH)
    pl.semaphore_signal(barrier, inc=1, device_id=(across, sp), device_id_type=MESH)
    pl.semaphore_signal(barrier, inc=1, device_id=(other, sp), device_id_type=MESH)
    for j in range(1, shards):
        there = lax.rem(sp + j, shards)
        pl.semaphore_signal(barrier, inc=1, device_id=(me, there), device_id_type=MESH)
        pl.semaphore_signal(barrier, inc=1, device_id=(other, there), device_id_type=MESH)

    def coef_copy(n):
        slot = lax.rem(n, 2)
        return pltpu.make_async_copy(coefs.at[0, pl.ds(n * CB, CB)], cbuf.at[slot], csem.at[slot])

    def weather_copy(n):
        return pltpu.make_async_copy(
            weather.at[0, pl.ds(n * CB, CB)], field.at[pl.ds(n * CB, CB)], wsem.at[n]
        )

    def out_copy(n):
        return pltpu.make_async_copy(
            field.at[pl.ds(n * CB, CB)], out.at[0, pl.ds(n * CB, CB)], osem.at[n]
        )

    coef_copy(0).start()
    coef_copy(1).start()
    for n in range(chunks):
        weather_copy(n).start()

    four[...] = jnp.zeros_like(four)
    nrow = order_local + 2
    m_row = (lax.broadcasted_iota(jnp.int32, (nrow, 128), 0) + sp * order_local).astype(F32)
    m_sq = m_row * m_row
    m_wide = jnp.concatenate([m_row, m_row], axis=1)
    cosine = jnp.broadcast_to(angle[0, 0:1, :], (nrow, lat))
    lsine = jnp.broadcast_to(angle[1, 0:1, :], (nrow, lat))
    dlog = diag[pl.ds(pl.multiple_of(sp * nrow, 8), nrow), :]
    first = jnp.exp(jnp.concatenate([dlog, dlog], axis=1) + m_wide * lsine)

    def block(b, carry):
        older, newer, q = carry
        for i in range(16):
            l = b * 16 + i
            lf = l.astype(F32)
            gap = lf * lf - m_sq
            r = lax.rsqrt(jnp.maximum(gap, 1.0))
            up = factors[0, l] * r
            down = factors[1, l] * q
            up2 = jnp.concatenate([up, up], axis=1)
            down2 = jnp.concatenate([down, down], axis=1)
            nxt = up2 * (cosine * newer - down2 * older)
            nxt = jnp.where(m_wide == lf, first, nxt)
            q = jnp.maximum(gap, 0.0) * r
            older, newer = newer, nxt
            for v in range(lat // 128):
                stage[v, pl.ds(i, nrow, stride=17), :] = nxt[:, 128 * v : 128 * v + 128]

        def put(m, c):
            for v in range(lat // 128):
                table[m, pl.ds(pl.multiple_of(b * 16, 16), 16), 128 * v : 128 * v + 128] = stage[
                    v, pl.ds(m * 17, 16), :
                ].astype(BF16)
            return c

        lax.fori_loop(0, order_local, put, 0, unroll=2)
        return older, newer, q

    empty = jnp.zeros((nrow, lat), F32)
    blocks = (degrees + 15) // 16
    lax.fori_loop(0, blocks, block, (empty, empty, jnp.zeros((nrow, 128), F32)))
    for m in range(order_local):
        if blocks * 16 < LPAD:
            table[m, blocks * 16 :, :] = jnp.zeros((LPAD - blocks * 16, lat), BF16)

    pl.semaphore_wait(barrier, 2 * (shards - 1) + 5)

    def make_basis():
        turn = [wave[2 + i] for i in range(4)]
        root2 = math.sqrt(2.0)

        def shard_rows(s, carry):
            u0, v0 = carry
            u, v = u0, v0
            for b in range(12):
                w = jnp.full((8, 1536), root2, F32)
                row = lax.broadcasted_iota(jnp.int32, (8, 1536), 0) + b * 8
                if b == 0:
                    w = jnp.where((row < 2) & (s == 0), 1.0, w)
                if b == 11:
                    w = jnp.where(row < 2 * order_local, w, 0.0)
                wide[pl.ds(b * 8, 8), :] = w * u
                u, v = u * turn[0] - v * turn[1], v * turn[0] + u * turn[1]
            basis[pl.ds(pl.multiple_of(s * 96, 16), 96), :] = wide[...].astype(BF16)
            return u0 * turn[2] - v0 * turn[3], v0 * turn[2] + u0 * turn[3]

        lax.fori_loop(0, shards, shard_rows, (wave[0], wave[1]))

    wide = rows
    make_basis()

    lane = lax.broadcasted_iota(jnp.int32, (8, 128), 1) // 32
    sub = lax.broadcasted_iota(jnp.int32, (8, 128), 0) // 2
    shift = lax.rem(lane - sub + 4, 4)
    masks = [shift == d for d in range(4)]
    degree_i = lax.broadcasted_iota(jnp.int32, (2 * CB, degrees), 1)

    def pair_copy(n):
        return pltpu.make_async_remote_copy(
            hsend.at[n], hrecv.at[n], hs.at[n], hr.at[n], device_id=(other, sp), device_id_type=MESH
        )

    def ring_copy(n, j):
        return pltpu.make_async_remote_copy(
            zsend.at[n, lax.rem(zpos + j, 4)], zrecv.at[n, j - 1], zs.at[n, j - 1], zr.at[n, j - 1],
            device_id=(ring[j], sp), device_id_type=MESH,
        )

    def across_copy(n):
        return pltpu.make_async_remote_copy(
            xsend.at[n], xrecv.at[n], xs.at[n], xr.at[n], device_id=(across, sp), device_id_type=MESH
        )

    def mean_copy(n, j):
        return pltpu.make_async_remote_copy(
            msend.at[n], mrecv.at[n, j - 1], ms.at[n, j - 1], mr.at[n, j - 1],
            device_id=(ring[j], sp), device_id_type=MESH,
        )

    def own_copy(n, i):
        return pltpu.make_async_remote_copy(
            aown.at[n, i], got.at[n, sp], sown.at[n, i], ar.at[n, sp],
            device_id=(me, mine + i), device_id_type=MESH,
        )

    def partner_copy(n, i):
        return pltpu.make_async_remote_copy(
            apar.at[n, i], got.at[n, sp], spar.at[n, i], ar.at[n, sp],
            device_id=(other, mine + i), device_id_type=MESH,
        )

    def arrival(n, s):
        return pltpu.make_async_remote_copy(
            aown.at[n, 0], got.at[n, s], sown.at[n, 0], ar.at[n, s],
            device_id=(other, sp), device_id_type=MESH,
        )

    def legendre(n):
        slot = lax.rem(n, 2)
        coef_copy(n).wait()

        def order(h, c):
            for e in range(2):
                m = h * 2 + e
                values = cbuf[slot, :, m].reshape(2 * CB, degrees).astype(F32) * factor
                lhs = jnp.where(degree_i >= sp * order_local + m, values, 0.0).astype(BF16)
                res = jnp.dot(lhs, table[m, 0:degrees, :], preferred_element_type=F32)
                for g in range(GR):
                    for v in range(lat // 128):
                        part = res[8 * g : 8 * g + 8, 128 * v : 128 * v + 128]
                        turned = part
                        for d in range(1, 4):
                            moved = pltpu.roll(pltpu.roll(part, 8 - 2 * d, 0), 32 * d, 1)
                            turned = jnp.where(masks[d], moved, turned)
                        for dd in range(4):
                            four[v * 4 + dd, g, pl.ds(h * 4 + 2 * e, 2), :] = turned[2 * dd : 2 * dd + 2, :]
            return c

        lax.fori_loop(0, order_local // 2, order, 0)
        @pl.when(n + 2 < chunks)
        def _():
            coef_copy(n + 2).start()

        for i in range(half):
            held[n, i] = four[mine + i].astype(BF16)
            hsend[n, i] = four[theirs + i].astype(BF16)
        pair_copy(n).start()

    def start_ring(n):
        pair_copy(n).wait_recv()
        for i in range(half):
            zsend[n, i] = (held[n, i].astype(F32) + hrecv[n, i].astype(F32)).astype(BF16)
        for j in (2, 1, 3):
            ring_copy(n, j).start()

    def start_across(n):
        total = zsend[n, zpos].astype(F32)
        for j in range(1, 4):
            ring_copy(n, j).wait_recv()
            total = total + zrecv[n, j - 1].astype(F32)
        xsend[n] = total.astype(BF16)
        across_copy(n).start()

    def start_mean(n):
        across_copy(n).wait_recv()
        total = xsend[n].astype(F32) + xrecv[n].astype(F32)
        msend[n] = (total * (1.0 / 16.0)).astype(BF16)
        for j in (2, 1, 3):
            mean_copy(n, j).start()

    def start_exchange(n):
        for j in range(4):
            i = lax.rem(zpos - j + 4, 4)
            if j == 0:
                mean = msend[n].astype(F32)
            else:
                mean_copy(n, j).wait_recv()
                mean = mrecv[n, j - 1].astype(F32)
            aown[n, i] = (held[n, i].astype(F32) - mean).astype(BF16)
            apar[n, i] = (hrecv[n, i].astype(F32) - mean).astype(BF16)
        for j in range(4):
            i = lax.rem(sp + 2 + j, 4)
            partner_copy(n, i).start()

            @pl.when(mine + i != sp)
            def _():
                own_copy(n, i).start()

            @pl.when(mine + i == sp)
            def _():
                got[n, sp] = aown[n, i]

    def finish(n):
        for s in range(shards):
            @pl.when(jnp.logical_or(s != sp, sp // half != core))
            def _():
                arrival(n, s).wait_recv()

        weather_copy(n).wait()
        lhs = []
        for g in range(GR):
            lhs.append(got[n, :, g].reshape(shards * 96, 128).T)
        lhs = jnp.concatenate(lhs, axis=0)
        for b in range(6):
            lo = b * 256
            width = min(256, lon - lo)
            res = jnp.dot(lhs, basis[:, lo : lo + 256], preferred_element_type=F32)
            for c in range(CB):
                k = n * CB + c
                old = field[k, :, lo : lo + width].astype(F32)
                field[k, :, lo : lo + width] = (
                    old + scale[k] * res[32 * c : 32 * c + 32, :width]
                ).astype(BF16)
        out_copy(n).start()

    def tick(n, carry):
        def stage_at(lag, f):
            @pl.when(jnp.logical_and(n >= lag, n < chunks + lag))
            def _():
                f(n - lag)

        stage_at(0, legendre)
        stage_at(1, start_across)
        stage_at(2, start_mean)
        stage_at(3, start_exchange)
        stage_at(0, start_ring)
        stage_at(4, finish)
        return carry

    lax.fori_loop(0, chunks + 4, tick, 0)

    def drain(n, carry):
        out_copy(n).wait()
        pair_copy(n).wait_send()
        across_copy(n).wait_send()
        for j in range(1, 4):
            ring_copy(n, j).wait_send()
            mean_copy(n, j).wait_send()
        for i in range(half):
            partner_copy(n, i).wait_send()

            @pl.when(mine + i != sp)
            def _():
                own_copy(n, i).wait_send()

        return carry

    lax.fori_loop(0, chunks, drain, 0)


def local(weather, coefficients, channel_scale):
    shards = lax.axis_size("space")
    _, channels, rows_local, lon = weather.shape
    order_local, degrees = coefficients.shape[3:]
    lat = rows_local * shards
    lat0 = (lon // 2 + 1 - lat) // 2
    chunks = channels // CB
    half = shards // 2
    factor = math.sqrt(3.0) * math.sqrt(4.0 * math.pi) / degrees * 2.0 ** (-30)
    diag, angle, factors, wave = seeds(order_local, shards, lat, lat0, lon)
    piece = (GR, 96, 128)
    V = pltpu.VMEM
    D = pltpu.SemaphoreType.DMA
    any_ = pl.BlockSpec(memory_space=pl.ANY)
    vmem = pl.BlockSpec(memory_space=pltpu.VMEM)
    smem = pl.BlockSpec(memory_space=pltpu.SMEM)
    dims = (chunks, order_local, degrees, lat, lon, shards, factor)
    return pl.pallas_call(
        functools.partial(kernel, dims),
        out_shape=jax.ShapeDtypeStruct(weather.shape, weather.dtype),
        in_specs=[any_, any_, smem, vmem, vmem, smem, vmem],
        out_specs=any_,
        scratch_shapes=[
            V((2, CB, order_local, 2, degrees), jnp.int32),
            V((lat // 128, (order_local + 2) * 17, 128), F32),
            V((order_local, LPAD, lat), BF16),
            V((shards,) + piece, F32),
            V((chunks, half) + piece, BF16),
            V((chunks, half) + piece, BF16),
            V((chunks, half) + piece, BF16),
            V((chunks, 4) + piece, BF16),
            V((chunks, 3) + piece, BF16),
            V((chunks,) + piece, BF16),
            V((chunks,) + piece, BF16),
            V((chunks,) + piece, BF16),
            V((chunks, 3) + piece, BF16),
            V((chunks, half) + piece, BF16),
            V((chunks, half) + piece, BF16),
            V((chunks, shards) + piece, BF16),
            V((96, 1536), F32),
            V((shards * 96, 1536), BF16),
            V((channels, rows_local, lon), BF16),
            D((2,)), D((chunks,)), D((chunks,)),
            D((chunks,)), D((chunks,)),
            D((chunks, 3)), D((chunks, 3)),
            D((chunks,)), D((chunks,)),
            D((chunks, 3)), D((chunks, 3)),
            D((chunks, half)), D((chunks, half)), D((chunks, shards)),
        ],
        compiler_params=pltpu.CompilerParams(
            collective_id=0, has_side_effects=True, vmem_limit_bytes=67043328
        ),
        name="synthesis",
    )(weather, coefficients.transpose(0, 1, 3, 2, 4), channel_scale, diag, angle, factors, wave)


def solution(mesh):
    return jax.shard_map(
        local,
        mesh=mesh,
        in_specs=(P("member", None, "space", None), P("member", None, None, "space", None), P()),
        out_specs=P("member", None, "space", None),
        check_vma=False,
    )
```

```python
import functools
import math

import jax
import jax.numpy as jnp
import numpy as np
from jax import lax
from jax.experimental import pallas as pl
from jax.experimental.pallas import tpu as pltpu
from jax.sharding import PartitionSpec as P

MESH = pl.DeviceIdType.MESH
F32 = jnp.float32
BF16 = jnp.bfloat16
CB = 12
GR = CB // 4
LPAD = 384
UNROLL = 23


def seeds(order_local, shards, lat, lat0, lon):
    rows = order_local + 2
    m_all = np.arange(shards * order_local + 8, dtype=np.float64)
    steps = np.maximum(m_all, 1.0)
    terms = np.where(m_all > 0, 0.5 * np.log((2.0 * steps + 1.0) / (2.0 * steps)), 0.0)
    logs = np.cumsum(terms) - 0.5 * math.log(4.0 * math.pi)
    index = order_local * np.arange(shards)[:, None] + np.arange(rows)[None, :]
    diag = np.broadcast_to(logs[index].reshape(-1, 1), (shards * rows, 128))
    colat = math.pi * (lat0 + np.arange(lat)) / (lon // 2)
    angle = np.broadcast_to(
        np.stack([np.cos(colat), np.log(np.sin(colat))])[:, None, :], (2, 8, lat)
    )
    degree = np.arange(LPAD, dtype=np.float64)
    factors = np.stack(
        [
            np.sqrt(np.maximum(4.0 * degree**2 - 1.0, 1.0)),
            1.0 / np.sqrt(np.maximum(4.0 * (degree - 1.0) ** 2 - 1.0, 1.0)),
        ]
    )
    lane = np.arange(1536)
    theta = np.where(lane < lon, 2.0 * math.pi * lane / lon, 0.0)[None, :]
    m = (np.arange(8) // 2)[:, None]
    p = (np.arange(8) % 2)[:, None]
    turn = []
    for by in (4, order_local):
        turn += [np.broadcast_to(f(by * theta), (8, 1536)) for f in (np.cos, np.sin)]
    wave = np.stack([np.cos(m * theta - p * math.pi / 2), np.sin(m * theta - p * math.pi / 2)] + turn)
    diag = diag.reshape(shards, rows, 128).transpose(1, 0, 2).reshape(rows, -1)
    lanes = np.repeat(factors.reshape(2, -1, 32).transpose(0, 2, 1), 128, axis=2).reshape(64, -1)
    tables = np.zeros((64 + rows + 64, 1536))
    tables[:48] = wave.reshape(48, 1536)
    tables[48:64, :lat] = angle.reshape(16, lat)
    tables[64 : 64 + rows, : diag.shape[1]] = diag
    tables[64 + rows :] = lanes
    return np.asarray(tables, np.float32)


def kernel(
    dims, weather, coefs, scale, tables, out,
    cbuf, stage, table, four, held, hsend, hrecv, zsend, zrecv, xsend, xrecv,
    msend, mrecv, aown, apar, got, rows, basis,
    csem, wsem, hs, hr, zs, zr, xs, xr, ms, mr, sown, spar, ar,
):
    chunks, order_local, degrees, lat, lon, shards, factor = dims
    half = shards // 2
    me = lax.axis_index("member")
    sp = lax.axis_index("space")
    core = lax.rem(me, 2)
    other = me + 1 - 2 * core
    across = me + 2 - 4 * lax.rem(me // 2, 2)
    zpos = me // 4
    ring = [lax.rem(zpos + j, 4) * 4 + lax.rem(me, 4) for j in range(4)]
    def band(c, i):
        return lax.rem(c + i // 2, 2) * half + i

    mine_is = lax.rem(sp // half + lax.rem(sp, half) // 2, 2) == core

    barrier = pltpu.get_barrier_semaphore()
    for j in range(1, 4):
        pl.semaphore_signal(barrier, inc=1, device_id=(ring[j], sp), device_id_type=MESH)
    pl.semaphore_signal(barrier, inc=1, device_id=(across, sp), device_id_type=MESH)
    pl.semaphore_signal(barrier, inc=1, device_id=(other, sp), device_id_type=MESH)
    for j in range(1, shards):
        there = lax.rem(sp + j, shards)
        pl.semaphore_signal(barrier, inc=1, device_id=(me, there), device_id_type=MESH)
        pl.semaphore_signal(barrier, inc=1, device_id=(other, there), device_id_type=MESH)

    def coef_copy(n):
        slot = lax.rem(n, 2)
        return pltpu.make_async_copy(coefs.at[0, pl.ds(n * CB, CB)], cbuf.at[slot], csem.at[slot])

    def weather_copy(n):
        return pltpu.make_async_copy(
            weather.at[0, pl.ds(n * CB, CB)], out.at[0, pl.ds(n * CB, CB)], wsem.at[n]
        )

    coef_copy(0).start()
    coef_copy(1).start()
    for n in range(chunks):
        weather_copy(n).start()

    four[...] = jnp.zeros_like(four)
    nrow = order_local + 2
    m_row = (lax.broadcasted_iota(jnp.int32, (nrow, 128), 0) + sp * order_local).astype(F32)
    m_sq = m_row * m_row
    m_wide = jnp.concatenate([m_row, m_row], axis=1)
    cosine = jnp.broadcast_to(tables[48:49, 0:lat], (nrow, lat))
    lsine = jnp.broadcast_to(tables[56:57, 0:lat], (nrow, lat))
    dlog = tables[64 : 64 + nrow, pl.ds(pl.multiple_of(sp * 128, 128), 128)]
    first = jnp.exp(jnp.concatenate([dlog, dlog], axis=1) + m_wide * lsine)

    def block(b, carry):
        older, newer, q = carry
        spot = pl.ds(pl.multiple_of(b // 2 * 128, 128), 128)
        line = 64 + nrow + lax.rem(b, 2) * 16
        ups = tables[pl.ds(pl.multiple_of(line, 8), 16), spot]
        downs = tables[pl.ds(pl.multiple_of(line + 32, 8), 16), spot]
        for i in range(16):
            l = b * 16 + i
            lf = l.astype(F32)
            gap = lf * lf - m_sq
            r = lax.rsqrt(jnp.maximum(gap, 1.0))
            up = ups[i : i + 1, :] * r
            down = downs[i : i + 1, :] * q
            up2 = jnp.concatenate([up, up], axis=1)
            down2 = jnp.concatenate([down, down], axis=1)
            nxt = up2 * (cosine * newer - down2 * older)
            nxt = jnp.where(m_wide == lf, first, nxt)
            q = jnp.maximum(gap, 0.0) * r
            older, newer = newer, nxt
            for v in range(lat // 128):
                stage[v, pl.ds(i, nrow, stride=17), :] = nxt[:, 128 * v : 128 * v + 128]

        def put(m, c):
            for v in range(lat // 128):
                table[m, pl.ds(pl.multiple_of(b * 16, 16), 16), 128 * v : 128 * v + 128] = stage[
                    v, pl.ds(m * 17, 16), :
                ].astype(BF16)
            return c

        lax.fori_loop(0, order_local, put, 0, unroll=2)
        return older, newer, q

    empty = jnp.zeros((nrow, lat), F32)
    blocks = (degrees + 15) // 16
    lax.fori_loop(0, blocks, block, (empty, empty, jnp.zeros((nrow, 128), F32)))
    for m in range(order_local):
        if blocks * 16 < LPAD:
            table[m, blocks * 16 :, :] = jnp.zeros((LPAD - blocks * 16, lat), BF16)

    pl.semaphore_wait(barrier, 2 * (shards - 1) + 5)

    def make_basis():
        turn = [tables[16 + 8 * i : 24 + 8 * i, :] for i in range(4)]
        root2 = math.sqrt(2.0)

        def shard_rows(s, carry):
            u0, v0 = carry
            u, v = u0, v0
            for b in range(12):
                w = jnp.full((8, 1536), root2, F32)
                row = lax.broadcasted_iota(jnp.int32, (8, 1536), 0) + b * 8
                if b == 0:
                    w = jnp.where((row < 2) & (s == 0), 1.0, w)
                if b == 11:
                    w = jnp.where(row < 2 * order_local, w, 0.0)
                wide[pl.ds(b * 8, 8), :] = w * u
                u, v = u * turn[0] - v * turn[1], v * turn[0] + u * turn[1]
            basis[pl.ds(pl.multiple_of(s * 96, 16), 96), :] = wide[...].astype(BF16)
            return u0 * turn[2] - v0 * turn[3], v0 * turn[2] + u0 * turn[3]

        lax.fori_loop(0, shards, shard_rows, (tables[0:8, :], tables[8:16, :]))

    wide = rows

    lane = lax.broadcasted_iota(jnp.int32, (8, 128), 1) // 32
    sub = lax.broadcasted_iota(jnp.int32, (8, 128), 0) // 2
    shift = lax.rem(lane - sub + 4, 4)
    masks = [shift == d for d in range(4)]
    degree_i = lax.broadcasted_iota(jnp.int32, (2 * CB, degrees), 1)

    def pair_copy(n):
        return pltpu.make_async_remote_copy(
            hsend.at[n], hrecv.at[n], hs.at[n], hr.at[n], device_id=(other, sp), device_id_type=MESH
        )

    def ring_copy(n, j):
        return pltpu.make_async_remote_copy(
            zsend.at[n, lax.rem(zpos + j, 4)], zrecv.at[n, j - 1], zs.at[n, j - 1], zr.at[n, j - 1],
            device_id=(ring[j], sp), device_id_type=MESH,
        )

    def across_copy(n):
        return pltpu.make_async_remote_copy(
            xsend.at[n], xrecv.at[n], xs.at[n], xr.at[n], device_id=(across, sp), device_id_type=MESH
        )

    def mean_copy(n, j):
        return pltpu.make_async_remote_copy(
            msend.at[n], mrecv.at[n, j - 1], ms.at[n, j - 1], mr.at[n, j - 1],
            device_id=(ring[j], sp), device_id_type=MESH,
        )

    def own_copy(n, i):
        return pltpu.make_async_remote_copy(
            aown.at[n, i], got.at[n, sp], sown.at[n, i], ar.at[n, sp],
            device_id=(me, band(core, i)), device_id_type=MESH,
        )

    def partner_copy(n, i):
        return pltpu.make_async_remote_copy(
            apar.at[n, i], got.at[n, sp], spar.at[n, i], ar.at[n, sp],
            device_id=(other, band(core, i)), device_id_type=MESH,
        )

    def arrival(n, s):
        return pltpu.make_async_remote_copy(
            aown.at[n, 0], got.at[n, s], sown.at[n, 0], ar.at[n, s],
            device_id=(other, sp), device_id_type=MESH,
        )

    def legendre(n):
        slot = lax.rem(n, 2)
        coef_copy(n).wait()

        def order(h, c):
            for e in range(UNROLL):
                m = h * UNROLL + e
                values = cbuf[slot, :, m].reshape(2 * CB, degrees).astype(F32) * factor
                lhs = jnp.where(degree_i >= sp * order_local + m, values, 0.0).astype(BF16)
                res = jnp.dot(lhs, table[m, 0:degrees, :], preferred_element_type=F32)
                for g in range(GR):
                    for v in range(lat // 128):
                        part = res[8 * g : 8 * g + 8, 128 * v : 128 * v + 128]
                        turned = part
                        for d in range(1, 4):
                            moved = pltpu.roll(pltpu.roll(part, 8 - 2 * d, 0), 32 * d, 1)
                            turned = jnp.where(masks[d], moved, turned)
                        for dd in range(4):
                            four[v * 4 + dd, g, pl.ds(2 * m, 2), :] = turned[2 * dd : 2 * dd + 2, :]
            return c

        lax.fori_loop(0, order_local // UNROLL, order, 0)
        @pl.when(n + 2 < chunks)
        def _():
            coef_copy(n + 2).start()

        for i in range(half):
            held[n, i] = four[band(core, i)].astype(BF16)
            hsend[n, i] = four[band(1 - core, i)].astype(BF16)
        pair_copy(n).start()

    def start_ring(n):
        pair_copy(n).wait_recv()
        for i in range(half):
            zsend[n, i] = (held[n, i].astype(F32) + hrecv[n, i].astype(F32)).astype(BF16)
        for j in (2, 1, 3):
            ring_copy(n, j).start()

    def start_across(n):
        total = zsend[n, zpos].astype(F32)
        for j in range(1, 4):
            ring_copy(n, j).wait_recv()
            total = total + zrecv[n, j - 1].astype(F32)
        xsend[n] = total.astype(BF16)
        across_copy(n).start()

    def start_mean(n):
        across_copy(n).wait_recv()
        total = xsend[n].astype(F32) + xrecv[n].astype(F32)
        msend[n] = (total * (1.0 / 16.0)).astype(BF16)
        for j in (2, 1, 3):
            mean_copy(n, j).start()

    def start_exchange(n):
        for j in range(4):
            i = lax.rem(zpos - j + 4, 4)
            if j == 0:
                mean = msend[n].astype(F32)
            else:
                mean_copy(n, j).wait_recv()
                mean = mrecv[n, j - 1].astype(F32)
            aown[n, i] = (held[n, i].astype(F32) - mean).astype(BF16)
            apar[n, i] = (hrecv[n, i].astype(F32) - mean).astype(BF16)
        for j in range(4):
            i = lax.rem(sp + 2 + j, 4)
            partner_copy(n, i).start()

            @pl.when(band(core, i) != sp)
            def _():
                own_copy(n, i).start()

            @pl.when(band(core, i) == sp)
            def _():
                got[n, sp] = aown[n, i]

    def finish(n):
        for s in range(shards):
            @pl.when(jnp.logical_or(s != sp, jnp.logical_not(mine_is)))
            def _():
                arrival(n, s).wait_recv()

        weather_copy(n).wait()
        lhs = []
        for g in range(GR):
            lhs.append(got[n, :, g].reshape(shards * 96, 128).T)
        lhs = jnp.concatenate(lhs, axis=0)
        for b in range(6):
            lo = b * 256
            width = min(256, lon - lo)
            res = jnp.dot(lhs, basis[:, lo : lo + 256], preferred_element_type=F32)
            for c in range(CB):
                k = n * CB + c
                old = out[0, k, :, lo : lo + width].astype(F32)
                out[0, k, :, lo : lo + width] = (
                    old + scale[k] * res[32 * c : 32 * c + 32, :width]
                ).astype(BF16)

    def tick(n, carry):
        def stage_at(lag, f):
            @pl.when(jnp.logical_and(n >= lag, n < chunks + lag))
            def _():
                f(n - lag)

        stage_at(1, start_ring)
        stage_at(2, start_across)
        stage_at(3, start_mean)
        stage_at(4, start_exchange)
        stage_at(0, legendre)

        @pl.when(n == 2)
        def _():
            make_basis()

        stage_at(5, finish)
        return carry

    lax.fori_loop(0, chunks + 5, tick, 0)

    def drain(n, carry):
        pair_copy(n).wait_send()
        across_copy(n).wait_send()
        for j in range(1, 4):
            ring_copy(n, j).wait_send()
            mean_copy(n, j).wait_send()
        for i in range(half):
            partner_copy(n, i).wait_send()

            @pl.when(band(core, i) != sp)
            def _():
                own_copy(n, i).wait_send()

        return carry

    lax.fori_loop(0, chunks, drain, 0)


def hand_over(array):
    pieces = 6
    step = array.shape[1] // pieces

    def body(src, dst, wsem):
        def store(i):
            part = pl.ds(i * step, step)
            return pltpu.make_async_copy(src.at[0, part], dst.at[0, part], wsem.at[i])

        for i in range(pieces):
            store(i).start()
        for i in range(pieces):
            store(i).wait()

    any_ = pl.BlockSpec(memory_space=pl.ANY)
    return pl.pallas_call(
        body,
        out_shape=jax.ShapeDtypeStruct(array.shape, array.dtype),
        in_specs=[pl.BlockSpec(memory_space=pltpu.VMEM)],
        out_specs=any_,
        scratch_shapes=[
            pltpu.SemaphoreType.DMA((pieces,)),
        ],
        compiler_params=pltpu.CompilerParams(vmem_limit_bytes=20 * 1024 * 1024),
        name="hand_over",
    )(array)


def local(weather, coefficients, channel_scale):
    shards = lax.axis_size("space")
    _, channels, rows_local, lon = weather.shape
    order_local, degrees = coefficients.shape[3:]
    lat = rows_local * shards
    lat0 = (lon // 2 + 1 - lat) // 2
    chunks = channels // CB
    half = shards // 2
    factor = math.sqrt(3.0) * math.sqrt(4.0 * math.pi) / degrees * 2.0 ** (-30)
    tables = seeds(order_local, shards, lat, lat0, lon)
    piece = (GR, 96, 128)
    V = pltpu.VMEM
    D = pltpu.SemaphoreType.DMA
    any_ = pl.BlockSpec(memory_space=pl.ANY)
    vmem = pl.BlockSpec(memory_space=pltpu.VMEM)
    smem = pl.BlockSpec(memory_space=pltpu.SMEM)
    dims = (chunks, order_local, degrees, lat, lon, shards, factor)
    result = pl.pallas_call(
        functools.partial(kernel, dims),
        out_shape=jax.ShapeDtypeStruct(weather.shape, weather.dtype),
        in_specs=[any_, any_, smem, vmem],
        out_specs=vmem,
        scratch_shapes=[
            V((2, CB, order_local, 2, degrees), jnp.int32),
            V((lat // 128, (order_local + 2) * 17, 128), F32),
            V((order_local, LPAD, lat), BF16),
            V((shards,) + piece, F32),
            V((chunks, half) + piece, BF16),
            V((chunks, half) + piece, BF16),
            V((chunks, half) + piece, BF16),
            V((chunks, 4) + piece, BF16),
            V((chunks, 3) + piece, BF16),
            V((chunks,) + piece, BF16),
            V((chunks,) + piece, BF16),
            V((chunks,) + piece, BF16),
            V((chunks, 3) + piece, BF16),
            V((chunks, half) + piece, BF16),
            V((chunks, half) + piece, BF16),
            V((chunks, shards) + piece, BF16),
            V((96, 1536), F32),
            V((shards * 96, 1536), BF16),
            D((2,)), D((chunks,)),
            D((chunks,)), D((chunks,)),
            D((chunks, 3)), D((chunks, 3)),
            D((chunks,)), D((chunks,)),
            D((chunks, 3)), D((chunks, 3)),
            D((chunks, half)), D((chunks, half)), D((chunks, shards)),
        ],
        compiler_params=pltpu.CompilerParams(
            collective_id=0, has_side_effects=True, vmem_limit_bytes=44 * 1024 * 1024
        ),
        name="synthesis",
    )(weather, coefficients.transpose(0, 1, 3, 2, 4), channel_scale, tables)
    return hand_over(result)


def solution(mesh):
    return jax.shard_map(
        local,
        mesh=mesh,
        in_specs=(P("member", None, "space", None), P("member", None, None, "space", None), P()),
        out_specs=P("member", None, "space", None),
        check_vma=False,
    )
```

```python
import functools
import math

import jax
import jax.numpy as jnp
import numpy as np
from jax import lax
from jax.experimental import pallas as pl
from jax.experimental.pallas import tpu as pltpu
from jax.sharding import PartitionSpec as P

MESH = pl.DeviceIdType.MESH
F32 = jnp.float32
BF16 = jnp.bfloat16
CB = 12
GR = CB // 4
LPAD = 384
UNROLL = 23
EARLY = 1


def seeds(order_local, shards, lat, lat0, lon):
    rows = order_local + 2
    m_all = np.arange(shards * order_local + 8, dtype=np.float64)
    steps = np.maximum(m_all, 1.0)
    terms = np.where(m_all > 0, 0.5 * np.log((2.0 * steps + 1.0) / (2.0 * steps)), 0.0)
    logs = np.cumsum(terms) - 0.5 * math.log(4.0 * math.pi)
    index = order_local * np.arange(shards)[:, None] + np.arange(rows)[None, :]
    diag = np.broadcast_to(logs[index].reshape(-1, 1), (shards * rows, 128))
    colat = math.pi * (lat0 + np.arange(lat)) / (lon // 2)
    angle = np.broadcast_to(
        np.stack([np.cos(colat), np.log(np.sin(colat))])[:, None, :], (2, 8, lat)
    )
    degree = np.arange(LPAD, dtype=np.float64)
    factors = np.stack(
        [
            np.sqrt(np.maximum(4.0 * degree**2 - 1.0, 1.0)),
            1.0 / np.sqrt(np.maximum(4.0 * (degree - 1.0) ** 2 - 1.0, 1.0)),
        ]
    )
    lane = np.arange(1536)
    theta = np.where(lane < lon, 2.0 * math.pi * lane / lon, 0.0)[None, :]
    m = (np.arange(8) // 2)[:, None]
    p = (np.arange(8) % 2)[:, None]
    turn = []
    for by in (4, order_local):
        turn += [np.broadcast_to(f(by * theta), (8, 1536)) for f in (np.cos, np.sin)]
    wave = np.stack([np.cos(m * theta - p * math.pi / 2), np.sin(m * theta - p * math.pi / 2)] + turn)
    diag = diag.reshape(shards, rows, 128).transpose(1, 0, 2).reshape(rows, -1)
    lanes = np.repeat(factors.reshape(2, -1, 32).transpose(0, 2, 1), 128, axis=2).reshape(64, -1)
    tables = np.zeros((64 + rows + 64, 1536))
    tables[:48] = wave.reshape(48, 1536)
    tables[48:64, :lat] = angle.reshape(16, lat)
    tables[64 : 64 + rows, : diag.shape[1]] = diag
    tables[64 + rows :] = lanes
    return np.asarray(tables, np.float32)


def kernel(
    dims, weather, coefs, scale, tables, out,
    cbuf, stage, table, four, held, hsend, hrecv, zsend, zrecv, xsend, xrecv,
    msend, mrecv, aown, apar, got, back, rows, basis,
    csem, wsem, hs, hr, zs, zr, xs, xr, ms, mr, sown, spar, ar, hs4, hr4, bs, br,
):
    chunks, order_local, degrees, lat, lon, shards, factor = dims
    half = shards // 2
    me = lax.axis_index("member")
    sp = lax.axis_index("space")
    core = lax.rem(me, 2)
    other = me + 1 - 2 * core
    across = me + 2 - 4 * lax.rem(me // 2, 2)
    zpos = me // 4
    ring = [lax.rem(zpos + j, 4) * 4 + lax.rem(me, 4) for j in range(4)]
    def band(c, i):
        return lax.rem(c + i // 2, 2) * half + i

    mine_is = lax.rem(sp // half + lax.rem(sp, half) // 2, 2) == core

    barrier = pltpu.get_barrier_semaphore()
    for j in range(1, 4):
        pl.semaphore_signal(barrier, inc=1, device_id=(ring[j], sp), device_id_type=MESH)
    pl.semaphore_signal(barrier, inc=1, device_id=(across, sp), device_id_type=MESH)
    pl.semaphore_signal(barrier, inc=1, device_id=(other, sp), device_id_type=MESH)
    for j in range(1, shards):
        there = lax.rem(sp + j, shards)
        pl.semaphore_signal(barrier, inc=1, device_id=(me, there), device_id_type=MESH)
        pl.semaphore_signal(barrier, inc=1, device_id=(other, there), device_id_type=MESH)

    def coef_copy(n):
        slot = lax.rem(n, 2)
        return pltpu.make_async_copy(coefs.at[0, pl.ds(n * CB, CB)], cbuf.at[slot], csem.at[slot])

    def weather_copy(n):
        return pltpu.make_async_copy(
            weather.at[0, pl.ds(n * CB, CB)], out.at[0, pl.ds(n * CB, CB)], wsem.at[n]
        )

    coef_copy(0).start()
    coef_copy(1).start()
    for n in range(chunks):
        weather_copy(n).start()

    four[...] = jnp.zeros_like(four)
    nrow = order_local + 2
    m_row = (lax.broadcasted_iota(jnp.int32, (nrow, 128), 0) + sp * order_local).astype(F32)
    m_sq = m_row * m_row
    m_wide = jnp.concatenate([m_row, m_row], axis=1)
    cosine = jnp.broadcast_to(tables[48:49, 0:lat], (nrow, lat))
    lsine = jnp.broadcast_to(tables[56:57, 0:lat], (nrow, lat))
    dlog = tables[64 : 64 + nrow, pl.ds(pl.multiple_of(sp * 128, 128), 128)]
    first = jnp.exp(jnp.concatenate([dlog, dlog], axis=1) + m_wide * lsine)

    def block(b, carry):
        older, newer, q = carry
        spot = pl.ds(pl.multiple_of(b // 2 * 128, 128), 128)
        line = 64 + nrow + lax.rem(b, 2) * 16
        ups = tables[pl.ds(pl.multiple_of(line, 8), 16), spot]
        downs = tables[pl.ds(pl.multiple_of(line + 32, 8), 16), spot]
        for i in range(16):
            l = b * 16 + i
            lf = l.astype(F32)
            gap = lf * lf - m_sq
            r = lax.rsqrt(jnp.maximum(gap, 1.0))
            up = ups[i : i + 1, :] * r
            down = downs[i : i + 1, :] * q
            up2 = jnp.concatenate([up, up], axis=1)
            down2 = jnp.concatenate([down, down], axis=1)
            nxt = up2 * (cosine * newer - down2 * older)
            nxt = jnp.where(m_wide == lf, first, nxt)
            q = jnp.maximum(gap, 0.0) * r
            older, newer = newer, nxt
            for v in range(lat // 128):
                stage[v, pl.ds(i, nrow, stride=17), :] = nxt[:, 128 * v : 128 * v + 128]

        def put(m, c):
            for v in range(lat // 128):
                table[m, pl.ds(pl.multiple_of(b * 16, 16), 16), 128 * v : 128 * v + 128] = stage[
                    v, pl.ds(m * 17, 16), :
                ].astype(BF16)
            return c

        lax.fori_loop(0, order_local, put, 0, unroll=2)
        return older, newer, q

    empty = jnp.zeros((nrow, lat), F32)
    blocks = (degrees + 15) // 16
    lax.fori_loop(0, blocks, block, (empty, empty, jnp.zeros((nrow, 128), F32)))
    for m in range(order_local):
        if blocks * 16 < LPAD:
            table[m, blocks * 16 :, :] = jnp.zeros((LPAD - blocks * 16, lat), BF16)

    pl.semaphore_wait(barrier, 2 * (shards - 1) + 5)

    def make_basis():
        turn = [tables[16 + 8 * i : 24 + 8 * i, :] for i in range(4)]
        root2 = math.sqrt(2.0)

        def shard_rows(s, carry):
            u0, v0 = carry
            u, v = u0, v0
            for b in range(12):
                w = jnp.full((8, 1536), root2, F32)
                row = lax.broadcasted_iota(jnp.int32, (8, 1536), 0) + b * 8
                if b == 0:
                    w = jnp.where((row < 2) & (s == 0), 1.0, w)
                if b == 11:
                    w = jnp.where(row < 2 * order_local, w, 0.0)
                wide[pl.ds(b * 8, 8), :] = w * u
                u, v = u * turn[0] - v * turn[1], v * turn[0] + u * turn[1]
            basis[pl.ds(pl.multiple_of(s * 96, 16), 96), :] = wide[...].astype(BF16)
            return u0 * turn[2] - v0 * turn[3], v0 * turn[2] + u0 * turn[3]

        lax.fori_loop(0, shards, shard_rows, (tables[0:8, :], tables[8:16, :]))

    wide = rows

    lane = lax.broadcasted_iota(jnp.int32, (8, 128), 1) // 32
    sub = lax.broadcasted_iota(jnp.int32, (8, 128), 0) // 2
    shift = lax.rem(lane - sub + 4, 4)
    masks = [shift == d for d in range(4)]
    degree_i = lax.broadcasted_iota(jnp.int32, (2 * CB, degrees), 1)

    def pair_copy(n):
        return pltpu.make_async_remote_copy(
            hsend.at[n], hrecv.at[n], hs.at[n], hr.at[n], device_id=(other, sp), device_id_type=MESH
        )

    def ring_copy(n, j):
        return pltpu.make_async_remote_copy(
            zsend.at[n, lax.rem(zpos + j, 4)], zrecv.at[n, j - 1], zs.at[n, j - 1], zr.at[n, j - 1],
            device_id=(ring[j], sp), device_id_type=MESH,
        )

    def across_copy(n):
        return pltpu.make_async_remote_copy(
            xsend.at[n], xrecv.at[n], xs.at[n], xr.at[n], device_id=(across, sp), device_id_type=MESH
        )

    def mean_copy(n, j):
        return pltpu.make_async_remote_copy(
            msend.at[n], mrecv.at[n, j - 1], ms.at[n, j - 1], mr.at[n, j - 1],
            device_id=(ring[j], sp), device_id_type=MESH,
        )

    def own_copy(n, i):
        return pltpu.make_async_remote_copy(
            aown.at[n, i], got.at[n, sp], sown.at[n, i], ar.at[n, sp],
            device_id=(me, band(core, i)), device_id_type=MESH,
        )

    def partner_copy(n, i):
        return pltpu.make_async_remote_copy(
            apar.at[n, i], got.at[n, sp], spar.at[n, i], ar.at[n, sp],
            device_id=(other, band(core, i)), device_id_type=MESH,
        )

    def arrival(n, s):
        return pltpu.make_async_remote_copy(
            aown.at[n, 0], got.at[n, s], sown.at[n, 0], ar.at[n, s],
            device_id=(other, sp), device_id_type=MESH,
        )

    def early(n):
        return jnp.logical_and(lax.rem(n, 2) == 0, n < EARLY)

    def raw_near(n, i):
        return pltpu.make_async_remote_copy(
            held.at[n, i], got.at[n, sp], sown.at[n, i], ar.at[n, sp],
            device_id=(me, band(core, i)), device_id_type=MESH,
        )

    def raw_far(n, i):
        return pltpu.make_async_remote_copy(
            hsend.at[n, i], got.at[n, sp], spar.at[n, i], ar.at[n, sp],
            device_id=(me, band(1 - core, i)), device_id_type=MESH,
        )

    def piece_copy(n, i):
        return pltpu.make_async_remote_copy(
            got.at[n, band(1 - core, i)], hrecv.at[n, i], hs4.at[n, i], hr4.at[n, i],
            device_id=(other, sp), device_id_type=MESH,
        )

    def return_copy(n, i):
        return pltpu.make_async_remote_copy(
            apar.at[n, i], back.at[n // 2, i], bs.at[n, i], br.at[n, i],
            device_id=(other, sp), device_id_type=MESH,
        )

    def start_pieces(n):
        for s in range(shards):
            @pl.when(s != sp)
            def _():
                arrival(n, s).wait_recv()

        for i in range(half):
            piece_copy(n, i).start()

    def start_early_ring(n):
        for i in range(half):
            piece_copy(n, i).wait_recv()
            total = got[n, band(core, i)].astype(F32) + hrecv[n, i].astype(F32)
            zsend[n, i] = total.astype(BF16)
        for j in (2, 1, 3):
            ring_copy(n, j).start()

    def start_return(n):
        for j in range(4):
            i = lax.rem(zpos - j + 4, 4)
            if j == 0:
                mean = msend[n].astype(F32)
            else:
                mean_copy(n, j).wait_recv()
                mean = mrecv[n, j - 1].astype(F32)
            at = band(core, i)
            got[n, at] = (got[n, at].astype(F32) - mean).astype(BF16)
            apar[n, i] = (hrecv[n, i].astype(F32) - mean).astype(BF16)
        for i in range(half):
            return_copy(n, i).start()

    def finish_early(n):
        for i in range(half):
            return_copy(n, i).wait_recv()
            piece_copy(n, i).wait_send()
            got[n, band(1 - core, i)] = back[n // 2, i]
        transform(n)

    def legendre(n):
        slot = lax.rem(n, 2)
        coef_copy(n).wait()

        def order(h, c):
            for e in range(UNROLL):
                m = h * UNROLL + e
                values = cbuf[slot, :, m].reshape(2 * CB, degrees).astype(F32) * factor
                lhs = jnp.where(degree_i >= sp * order_local + m, values, 0.0).astype(BF16)
                res = jnp.dot(lhs, table[m, 0:degrees, :], preferred_element_type=F32)
                for g in range(GR):
                    for v in range(lat // 128):
                        part = res[8 * g : 8 * g + 8, 128 * v : 128 * v + 128]
                        turned = part
                        for d in range(1, 4):
                            moved = pltpu.roll(pltpu.roll(part, 8 - 2 * d, 0), 32 * d, 1)
                            turned = jnp.where(masks[d], moved, turned)
                        for dd in range(4):
                            four[v * 4 + dd, g, pl.ds(2 * m, 2), :] = turned[2 * dd : 2 * dd + 2, :]
            return c

        lax.fori_loop(0, order_local // UNROLL, order, 0)
        @pl.when(n + 2 < chunks)
        def _():
            coef_copy(n + 2).start()

        for i in range(half):
            held[n, i] = four[band(core, i)].astype(BF16)
            hsend[n, i] = four[band(1 - core, i)].astype(BF16)

        @pl.when(jnp.logical_not(early(n)))
        def _():
            pair_copy(n).start()

        @pl.when(early(n))
        def _():
            for j in range(half):
                i = lax.rem(sp + 2 + j, half)
                for raw, to, src in (
                    (raw_far, band(1 - core, i), hsend),
                    (raw_near, band(core, i), held),
                ):
                    @pl.when(to != sp)
                    def _():
                        raw(n, i).start()

                    @pl.when(to == sp)
                    def _():
                        got[n, sp] = src[n, i]

    def start_ring(n):
        pair_copy(n).wait_recv()
        for i in range(half):
            zsend[n, i] = (held[n, i].astype(F32) + hrecv[n, i].astype(F32)).astype(BF16)
        for j in (2, 1, 3):
            ring_copy(n, j).start()

    def start_across(n):
        total = zsend[n, zpos].astype(F32)
        for j in range(1, 4):
            ring_copy(n, j).wait_recv()
            total = total + zrecv[n, j - 1].astype(F32)
        xsend[n] = total.astype(BF16)
        across_copy(n).start()

    def start_mean(n):
        across_copy(n).wait_recv()
        total = xsend[n].astype(F32) + xrecv[n].astype(F32)
        msend[n] = (total * (1.0 / 16.0)).astype(BF16)
        for j in (2, 1, 3):
            mean_copy(n, j).start()

    def start_exchange(n):
        for j in range(4):
            i = lax.rem(zpos - j + 4, 4)
            if j == 0:
                mean = msend[n].astype(F32)
            else:
                mean_copy(n, j).wait_recv()
                mean = mrecv[n, j - 1].astype(F32)
            aown[n, i] = (held[n, i].astype(F32) - mean).astype(BF16)
            apar[n, i] = (hrecv[n, i].astype(F32) - mean).astype(BF16)
        for j in range(4):
            i = lax.rem(sp + 2 + j, 4)
            partner_copy(n, i).start()

            @pl.when(band(core, i) != sp)
            def _():
                own_copy(n, i).start()

            @pl.when(band(core, i) == sp)
            def _():
                got[n, sp] = aown[n, i]

    def finish(n):
        for s in range(shards):
            @pl.when(jnp.logical_or(s != sp, jnp.logical_not(mine_is)))
            def _():
                arrival(n, s).wait_recv()

        transform(n)

    def transform(n):
        weather_copy(n).wait()
        lhs = []
        for g in range(GR):
            lhs.append(got[n, :, g].reshape(shards * 96, 128).T)
        lhs = jnp.concatenate(lhs, axis=0)
        for b in range(6):
            lo = b * 256
            width = min(256, lon - lo)
            res = jnp.dot(lhs, basis[:, lo : lo + 256], preferred_element_type=F32)
            for c in range(CB):
                k = n * CB + c
                old = out[0, k, :, lo : lo + width].astype(F32)
                out[0, k, :, lo : lo + width] = (
                    old + scale[k] * res[32 * c : 32 * c + 32, :width]
                ).astype(BF16)

    def tick(n, carry):
        def stage_at(lag, f, kind=None):
            k = n - lag
            on = jnp.logical_and(k >= 0, k < chunks)
            if kind is not None:
                on = jnp.logical_and(on, early(k) if kind else jnp.logical_not(early(k)))

            @pl.when(on)
            def _():
                f(k)

        stage_at(1, start_ring, False)
        stage_at(6, start_early_ring, True)
        stage_at(2, start_across, False)
        stage_at(7, start_across, True)
        stage_at(3, start_mean, False)
        stage_at(8, start_mean, True)
        stage_at(4, start_exchange, False)
        stage_at(9, start_return, True)
        stage_at(0, legendre)

        @pl.when(n == 2)
        def _():
            make_basis()

        stage_at(5, start_pieces, True)
        stage_at(5, finish, False)
        stage_at(10, finish_early, True)
        return carry

    lax.fori_loop(0, max(chunks + 5, EARLY + 10), tick, 0)

    def drain(n, carry):
        across_copy(n).wait_send()
        for j in range(1, 4):
            ring_copy(n, j).wait_send()
            mean_copy(n, j).wait_send()

        @pl.when(jnp.logical_not(early(n)))
        def _():
            pair_copy(n).wait_send()
            for i in range(half):
                partner_copy(n, i).wait_send()

                @pl.when(band(core, i) != sp)
                def _():
                    own_copy(n, i).wait_send()

        @pl.when(early(n))
        def _():
            for i in range(half):
                return_copy(n, i).wait_send()

                @pl.when(band(core, i) != sp)
                def _():
                    raw_near(n, i).wait_send()

                @pl.when(band(1 - core, i) != sp)
                def _():
                    raw_far(n, i).wait_send()

        return carry

    lax.fori_loop(0, chunks, drain, 0)


def hand_over(array):
    pieces = 6
    step = array.shape[1] // pieces

    def body(src, dst, wsem):
        def store(i):
            part = pl.ds(i * step, step)
            return pltpu.make_async_copy(src.at[0, part], dst.at[0, part], wsem.at[i])

        for i in range(pieces):
            store(i).start()
        for i in range(pieces):
            store(i).wait()

    any_ = pl.BlockSpec(memory_space=pl.ANY)
    return pl.pallas_call(
        body,
        out_shape=jax.ShapeDtypeStruct(array.shape, array.dtype),
        in_specs=[pl.BlockSpec(memory_space=pltpu.VMEM)],
        out_specs=any_,
        scratch_shapes=[
            pltpu.SemaphoreType.DMA((pieces,)),
        ],
        compiler_params=pltpu.CompilerParams(vmem_limit_bytes=20 * 1024 * 1024),
        name="hand_over",
    )(array)


def local(weather, coefficients, channel_scale):
    shards = lax.axis_size("space")
    _, channels, rows_local, lon = weather.shape
    order_local, degrees = coefficients.shape[3:]
    lat = rows_local * shards
    lat0 = (lon // 2 + 1 - lat) // 2
    chunks = channels // CB
    half = shards // 2
    factor = math.sqrt(3.0) * math.sqrt(4.0 * math.pi) / degrees * 2.0 ** (-30)
    tables = seeds(order_local, shards, lat, lat0, lon)
    piece = (GR, 96, 128)
    V = pltpu.VMEM
    D = pltpu.SemaphoreType.DMA
    any_ = pl.BlockSpec(memory_space=pl.ANY)
    vmem = pl.BlockSpec(memory_space=pltpu.VMEM)
    smem = pl.BlockSpec(memory_space=pltpu.SMEM)
    dims = (chunks, order_local, degrees, lat, lon, shards, factor)
    result = pl.pallas_call(
        functools.partial(kernel, dims),
        out_shape=jax.ShapeDtypeStruct(weather.shape, weather.dtype),
        in_specs=[any_, any_, smem, vmem],
        out_specs=vmem,
        scratch_shapes=[
            V((2, CB, order_local, 2, degrees), jnp.int32),
            V((lat // 128, (order_local + 2) * 17, 128), F32),
            V((order_local, LPAD, lat), BF16),
            V((shards,) + piece, F32),
            V((chunks, half) + piece, BF16),
            V((chunks, half) + piece, BF16),
            V((chunks, half) + piece, BF16),
            V((chunks, 4) + piece, BF16),
            V((chunks, 3) + piece, BF16),
            V((chunks,) + piece, BF16),
            V((chunks,) + piece, BF16),
            V((chunks,) + piece, BF16),
            V((chunks, 3) + piece, BF16),
            V((chunks, half) + piece, BF16),
            V((chunks, half) + piece, BF16),
            V((chunks, shards) + piece, BF16),
            V(((EARLY + 1) // 2, half) + piece, BF16),
            V((96, 1536), F32),
            V((shards * 96, 1536), BF16),
            D((2,)), D((chunks,)),
            D((chunks,)), D((chunks,)),
            D((chunks, 3)), D((chunks, 3)),
            D((chunks,)), D((chunks,)),
            D((chunks, 3)), D((chunks, 3)),
            D((chunks, half)), D((chunks, half)), D((chunks, shards)),
            D((chunks, half)), D((chunks, half)), D((chunks, half)), D((chunks, half)),
        ],
        compiler_params=pltpu.CompilerParams(
            collective_id=0, has_side_effects=True, vmem_limit_bytes=44 * 1024 * 1024
        ),
        name="synthesis",
    )(weather, coefficients.transpose(0, 1, 3, 2, 4), channel_scale, tables)
    return hand_over(result)


def solution(mesh):
    return jax.shard_map(
        local,
        mesh=mesh,
        in_specs=(P("member", None, "space", None), P("member", None, None, "space", None), P()),
        out_specs=P("member", None, "space", None),
        check_vma=False,
    )
```
